32 devices in a mesh: dp: 4 (over y, z), tp: 8 (over x, core).
Axes of the slice: x: 4, y: 2, z: 2, core: 2. Of those that a mesh axis runs over, the one named last changes fastest.
The devices are a block of a 4x4x8 slice.
Arguments:
- ids: int32 [64, 256], P('dp'), parts along dimension 0
- E: bfloat16 [4096, 4096], P(None, 'tp')
- g: bfloat16 [4096], replicated
- W: bfloat16 [4096, 6144], P(None, 'tp')
- du: bfloat16 [64, 256, 6144], P('dp', None, 'tp'), parts along dimension 0
- dres: bfloat16 [64, 256, 4096], P('dp', 'tp'), parts along dimension 0
Outputs:
- output 1: bfloat16 [64, 256, 6144], P('dp', None, 'tp'), parts along dimension 0
- output 2: bfloat16 [64, 256, 4096], P('dp', 'tp'), parts along dimension 0
- output 3: float32 [16384, 4096], P('dp', 'tp'), parts along dimension 0
- output 4: float32 [16384, 6144], P('dp', 'tp'), parts along dimension 0
- output 5: float32 [16384], P('dp'), parts along dimension 0
There are 4 independent parts. The reference program is written for one: setup_inputs(seed, part) draws one part's arguments, and reference() takes and returns one part's arrays. A program takes and returns all parts, laid end to end along the dimension named above; an argument that names none is the same for every part.
All inputs are finite; a program needn't handle non-finite values.
Results may differ from the reference program's by a relative error of at most 0.00617823.
Values are sent between devices in bfloat16 or wider.
A program may use at most 768 MiB of HBM per device.

```python
import jax
import jax.numpy as jnp
from jax import lax
import math

K = 16
T = 256
V = 4096
D = 4096
FC = 6144
EPS = 1e-6


def setup_inputs(seed: int = 0, part: int = 0) -> dict:
    key = jax.random.key(seed)
    kE, kg, kW, kpart = jax.random.split(key, 4)
    kp = jax.random.fold_in(kpart, part)
    k1, k2, k3, k4, k5, k6 = jax.random.split(kp, 6)
    scale = 1.0 / math.sqrt(K * T)
    dscale = scale * math.sqrt(D / FC)
    wscale = 1.0 / math.sqrt(D)
    E = jax.random.normal(kE, (V, D), jnp.float32).astype(jnp.bfloat16)
    g = (1.0 + 0.4 * jax.random.normal(kg, (D,), jnp.float32)).astype(jnp.bfloat16)
    W = (jax.random.normal(kW, (D, FC), jnp.float32) * wscale).astype(jnp.bfloat16)
    rand_bits = jax.random.bits(jax.random.fold_in(k1, 7), (K, T), jnp.uint32) >> 16
    square_part = (rand_bits * rand_bits) >> 16
    fourth_power = (square_part * square_part) >> 16
    ids = jnp.minimum(((fourth_power * (V >> 6)) >> 10).astype(jnp.int32), V - 1)
    du = (jax.random.normal(k5, (K, T, FC), jnp.float32) * dscale).astype(jnp.bfloat16)
    dres = (jax.random.normal(k6, (K, T, D), jnp.float32) * scale).astype(jnp.bfloat16)
    return dict(ids=ids, E=E, g=g, W=W, du=du, dres=dres)


def reference(ids, E, g, W, du, dres):
    gf = g.astype(jnp.float32)

    def step(carry, inp):
        dE, dW, dg = carry
        idk, duk, dresk = inp
        x = jnp.take(E, idk, axis=0)
        xf = x.astype(jnp.float32)
        rs = lax.rsqrt(jnp.mean(xf * xf, axis=-1, keepdims=True) + EPS)
        nh = xf * rs
        n = (nh * gf).astype(jnp.bfloat16)
        u = jnp.dot(n, W, preferred_element_type=jnp.float32).astype(jnp.bfloat16)
        dn = jnp.dot(duk, W.T, preferred_element_type=jnp.float32)
        gdn = gf * dn
        dx = dresk.astype(jnp.float32) + rs * (gdn - nh * jnp.mean(nh * gdn, axis=-1, keepdims=True))
        dE = dE.at[idk].add(dx)
        dW = dW + jnp.dot(n.T, duk, preferred_element_type=jnp.float32)
        dg = dg + jnp.sum(dn * nh, axis=0)
        return (dE, dW, dg), (u, x)

    init = (jnp.zeros((V, D), jnp.float32), jnp.zeros((D, FC), jnp.float32), jnp.zeros((D,), jnp.float32))
    (dE, dW, dg), (u, x) = lax.scan(step, init, (ids, du, dres))
    return u, x, dE, dW, dg
```

```python
import functools

import jax
import jax.numpy as jnp
from jax import lax
from jax.experimental import pallas as pl
from jax.experimental.pallas import tpu as pltpu
from jax.sharding import PartitionSpec as P

EPS = 1e-6
TM = 512
f32, bf16 = jnp.float32, jnp.bfloat16
MESH = pl.DeviceIdType.MESH


def kernel(G, DN, ids_col, ids_row, g8, E, W, du, dr,
           u_o, x_o, dE_o, dW_o, dg_o,
           xbuf, dup, drw, dst, pf0, pb, rb, st,
           E_v, W_v, wp_v, dW_v, dE_v, rs_v, acc_v, accu_v, d3_v, drl_v,
           s_loc, s_rcv, sm_v, dg_loc, dg_all, lsem, ssem, rsem):
    C = G // 2
    K, TL, D = dr.shape
    N, FL = du.shape
    V, DL = E.shape
    T = TL * G
    NTILE = N // TM
    MT = TM // T
    r = lax.axis_index('tp')
    k, c = lax.div(r, 2), lax.rem(r, 2)
    mate = r + 1 - 2 * c
    right = lax.rem(r + 2, G)
    left = lax.rem(r + G - 2, G)

    def blk(o, p):
        return lax.rem(k + o, C) * 2 + (c if p == 0 else 1 - c)

    def cols(b, n=DL):
        return pl.ds(pl.multiple_of(b * DL, DL), n)

    used = [0]

    def rcopy(src, dstr, dev):
        i = used[0]
        used[0] += 1
        return pltpu.make_async_remote_copy(
            src_ref=src, dst_ref=dstr, send_sem=ssem.at[i], recv_sem=rsem.at[i],
            device_id={'tp': dev}, device_id_type=MESH)

    sent = []

    def start(cp):
        cp.start()
        sent.append(cp)
        return cp

    barrier = pltpu.get_barrier_semaphore()
    for d in range(1, G):
        pl.semaphore_signal(barrier, inc=1, device_id={'tp': lax.rem(r + d, G)}, device_id_type=MESH)
    pl.semaphore_wait(barrier, G - 1)

    rows = pl.ds(pl.multiple_of(r * TL, TL), TL)
    Kh = K // 2
    dres_in = []
    to_r = start(rcopy(dr.at[pl.ds(0, Kh), :, cols(lax.rem(k + 2, C) * 2, 2 * DL)], dst.at[0], right))
    to_l = start(rcopy(dr.at[pl.ds(Kh, Kh), :, cols(lax.rem(k + 2, C) * 2, 2 * DL)], dst.at[1], left))
    for o in (1, C - 1):
        for p in range(2):
            b = blk(o, p)
            dres_in.append(start(rcopy(dr.at[:, :, cols(b)], drw.at[:, rows, :], b)))
    dup_cp = start(rcopy(du, dup, mate))
    wp_cp = [start(rcopy(W.at[cols(blk(o, 1)), :], wp_v.at[o], mate)) for o in range(C)]
    dres_in.append(start(rcopy(dr.at[:, :, cols(mate)], drw.at[:, rows, :], mate)))

    cE = pltpu.make_async_copy(E, E_v, lsem.at[0])
    cW = pltpu.make_async_copy(W, W_v, lsem.at[1])
    cD = pltpu.make_async_copy(dr.at[:, :, cols(r)], drl_v, lsem.at[2])
    cE.start()
    cW.start()
    cD.start()
    cE.wait()

    NA = 2
    NT = N // NA
    h = NT // 2
    TA = NT // TM

    def gather(step, id_b, xl_b):
        acc_v[...] = jnp.zeros_like(acc_v)

        @pl.loop(0, V // TM)
        def _(v):
            it = lax.broadcasted_iota(jnp.int32, (TM, TM), 1) + v * TM
            oh = jnp.where(id_b[...] == it, 1.0, 0.0).astype(bf16)
            acc_v[...] += jnp.dot(oh, E_v[pl.ds(pl.multiple_of(v * TM, TM), TM), :], preferred_element_type=f32)

        xl_b[...] = acc_v[...].astype(bf16)

    x_first = []
    for i in range(NA):
        pltpu.emit_pipeline(
            gather, grid=(TA,),
            in_specs=[pl.BlockSpec((TM, 1), lambda t, i=i: (t + i * TA, 0))],
            out_specs=[pl.BlockSpec((TM, DL), lambda t, i=i: (t + i * TA, 0))],
            _explicit_indices=True,
        )(ids_col, xbuf.at[0])
        cs = pl.ds(i * NT, NT)
        x_first.append((
            start(rcopy(xbuf.at[0, cs], xbuf.at[6, cs], right)),
            start(rcopy(xbuf.at[0, cs], xbuf.at[2, cs], left)),
            start(rcopy(xbuf.at[0, cs], xbuf.at[1, cs], mate))))

    cD.wait()
    cD2 = pltpu.make_async_copy(drl_v, drw.at[:, rows, :], lsem.at[2])
    cD2.start()
    dW_v[...] = jnp.zeros_like(dW_v)
    dE_v[...] = jnp.zeros_like(dE_v)
    dg_loc[...] = jnp.zeros_like(dg_loc)

    to_r.wait_recv()
    rl = pl.ds(pl.multiple_of(left * TL, TL), TL)
    rr = pl.ds(pl.multiple_of(right * TL, TL), TL)
    for p in range(2):
        q = c if p == 0 else 1 - c
        dres_in.append(start(rcopy(dst.at[0, :, :, pl.ds(pl.multiple_of(q * DL, DL), DL)],
                                   drw.at[pl.ds(0, Kh), rl, :], lax.rem(k + 1, C) * 2 + q)))
    to_l.wait_recv()
    for p in range(2):
        q = c if p == 0 else 1 - c
        dres_in.append(start(rcopy(dst.at[1, :, :, pl.ds(pl.multiple_of(q * DL, DL), DL)],
                                   drw.at[pl.ds(Kh, Kh), rr, :], lax.rem(k + C - 1, C) * 2 + q)))

    cW.wait()
    dup_cp.wait_recv()
    for cp in wp_cp:
        cp.wait_recv()
    nt_dims = (((1,), (1,)), ((), ()))

    def partial(step, du_b, dp_b, p0_b, p_b):
        for o in range(C):
            w = W_v[cols(blk(o, 0)), :]
            a = lax.dot_general(du_b[...], w, nt_dims, preferred_element_type=f32)
            a = a + lax.dot_general(dp_b[...], wp_v[o], nt_dims, preferred_element_type=f32)
            if o == 0:
                p0_b[...] = a
            else:
                p_b[o - 1] = a.astype(bf16)

    tile = lambda t: (t, 0)
    pltpu.emit_pipeline(
        partial, grid=(NTILE,),
        in_specs=[pl.BlockSpec((TM, FL), tile), pl.BlockSpec((TM, FL), tile)],
        out_specs=[pl.BlockSpec((TM, DL), tile), pl.BlockSpec((C - 1, TM, DL), lambda t: (0, t, 0))],
        _explicit_indices=True,
    )(du, dup, pf0, pb)

    x_second, x_mate = [], []
    for i in range(NA):
        fr, fl, _ = x_first[i]
        lo, hi = pl.ds(i * NT, h), pl.ds(i * NT + h, h)
        cs = pl.ds(i * NT, NT)
        fr.wait_recv()
        a = start(rcopy(xbuf.at[6, lo], xbuf.at[4, lo], right))
        m6 = start(rcopy(xbuf.at[6, cs], xbuf.at[7, cs], mate))
        fl.wait_recv()
        b = start(rcopy(xbuf.at[2, hi], xbuf.at[4, hi], left))
        m2 = start(rcopy(xbuf.at[2, cs], xbuf.at[3, cs], mate))
        x_second.append((a, b))
        x_mate.append([m6, m2])

    def dn_send(i):
        t0, n = DN[i]
        lo, hi = pl.ds(t0 * TM, n * TM // 2), pl.ds(t0 * TM + n * TM // 2, n * TM // 2)
        cs = pl.ds(t0 * TM, n * TM)
        return (start(rcopy(pb.at[0, cs], rb.at[2, cs], right)),
                start(rcopy(pb.at[2, cs], rb.at[0, cs], left)),
                start(rcopy(pb.at[1, lo], st.at[lo], right)),
                start(rcopy(pb.at[1, hi], st.at[hi], left)), lo, hi)

    def dn_forward(q):
        a, b, ra, rbk, lo, hi = q
        ra.wait_recv()
        f1 = start(rcopy(st.at[lo], rb.at[1, lo], right))
        rbk.wait_recv()
        f2 = start(rcopy(st.at[hi], rb.at[1, hi], left))
        return a, b, f1, f2

    first = [dn_send(0), dn_send(1)]

    t_dims = (((0,), (0,)), ((), ()))

    def forward(step, i, x_b, du_b, u_b, xo_b):
        t = step.index[0] + i * TA
        rs_v[pl.ds(pl.multiple_of(t * TM, TM), TM), :] = jnp.zeros((TM, 1), f32)
        here = pl.ds(pl.multiple_of(t * TM, TM), TM)

        @pl.loop(0, G)
        def _(j):
            x = x_b[j].astype(f32)
            rs_v[here, :] += jnp.sum(x * x, axis=-1, keepdims=True)

        rs_v[here, :] = lax.rsqrt(rs_v[here, :] / D + EPS)
        accu_v[...] = jnp.zeros_like(accu_v)

        @pl.loop(0, G)
        def _(j):
            p = lax.rem(j, 2)
            b = lax.rem(k + lax.div(j, 2), C) * 2 + c + p - 2 * c * p
            n = ((x_b[j].astype(f32) * rs_v[here, :]) * g8[pl.ds(b, 1), :]).astype(bf16)
            accu_v[...] += jnp.dot(n, W_v[cols(b), :], preferred_element_type=f32)
            dW_v[cols(b), :] += lax.dot_general(n, du_b[...], t_dims, preferred_element_type=f32)
            for m in range(MT):
                xo_b[m, :, cols(b)] = x_b[j, pl.ds(pl.multiple_of(m * T + r * TL, TL), TL), :]

        uf = accu_v[...]
        u_b[...] = uf.astype(bf16)
        s = jnp.sum(uf * du_b[...].astype(f32), axis=-1, keepdims=True)
        s_loc[pl.ds(t, 1), :] = jnp.broadcast_to(s, (TM, 128)).T[0:1, :]

    for i in range(NA):
        a, b = x_second[i]
        lo, hi = pl.ds(i * NT, h), pl.ds(i * NT + h, h)
        a.wait_recv()
        m4a = start(rcopy(xbuf.at[4, lo], xbuf.at[5, lo], mate))
        b.wait_recv()
        m4b = start(rcopy(xbuf.at[4, hi], xbuf.at[5, hi], mate))
        x_first[i][2].wait_recv()
        for cp in x_mate[i]:
            cp.wait_recv()
        m4a.wait_recv()
        m4b.wait_recv()
        at = lambda t, i=i: (t + i * TA, 0)
        pltpu.emit_pipeline(
            lambda step, *refs, i=i: forward(step, i, *refs), grid=(TA,),
            in_specs=[pl.BlockSpec((G, TM, DL), lambda t, i=i: (0, t + i * TA, 0)), pl.BlockSpec((TM, FL), at)],
            out_specs=[pl.BlockSpec((TM, FL), at), pl.BlockSpec((MT, TL, D), lambda t, i=i: (t + i * TA, 0, 0))],
            _explicit_indices=True,
        )(xbuf, du, u_o, x_o)

    cdW = pltpu.make_async_copy(dW_v, dW_o, lsem.at[3])
    cdW.start()
    s_cp = [start(rcopy(s_loc, s_rcv.at[G - d - 1], lax.rem(r + d, G))) for d in range(1, G)]
    done = [dn_forward(first[0])]
    rest = [dn_send(i) for i in range(2, len(DN))]
    for cp in s_cp:
        cp.wait_recv()
    tot = jnp.zeros_like(s_loc)
    for dev in range(G):
        d = lax.rem(dev - r + G, G)
        other = s_rcv[lax.max(d - 1, 0)]
        tot = tot + jnp.where(d == 0, s_loc[...], other)
    sm_v[...] = tot / D
    done.append(dn_forward(first[1]))
    cD2.wait()
    for cp in dres_in:
        cp.wait_recv()

    def backward(step, t0, p0_b, rb_b, xl_b, dr_b):
        t = step.index[0] + t0
        here = pl.ds(pl.multiple_of(t * TM, TM), TM)
        dn = (p0_b[...] + rb_b[0].astype(f32)) + (rb_b[1].astype(f32) + rb_b[2].astype(f32))
        rs = rs_v[here, :]
        s = jnp.broadcast_to(sm_v[pl.ds(t, 1), :], (128, TM)).T[:, 0:1]
        nh = xl_b[...].astype(f32) * rs
        dx = dr_b[...].reshape(TM, DL).astype(f32) + rs * (g8[pl.ds(r, 1), :] * dn - nh * s)
        dg_loc[0:1, :] += jnp.sum(dn * nh, axis=0, keepdims=True)
        hi = dx.astype(bf16)
        e1 = dx - hi.astype(f32)
        md = e1.astype(bf16)
        d3_v[0] = hi
        d3_v[1] = md
        d3_v[2] = (e1 - md.astype(f32)).astype(bf16)

        @pl.loop(0, V // TM)
        def _(v):
            it = lax.broadcasted_iota(jnp.int32, (TM, TM), 0) + v * TM
            oh = jnp.where(ids_row[pl.ds(t, 1), :] == it, 1.0, 0.0).astype(bf16)
            a = jnp.dot(oh, d3_v[0], preferred_element_type=f32)
            a = a + jnp.dot(oh, d3_v[1], preferred_element_type=f32)
            a = a + jnp.dot(oh, d3_v[2], preferred_element_type=f32)
            dE_v[pl.ds(pl.multiple_of(v * TM, TM), TM), :] += a

    for i, (t0, n) in enumerate(DN):
        if i >= 2:
            pass
        a, b, f1, f2 = done[i]
        a.wait_recv()
        b.wait_recv()
        f1.wait_recv()
        f2.wait_recv()
        at = lambda t, t0=t0: (t + t0, 0)
        pltpu.emit_pipeline(
            lambda step, *refs, t0=t0: backward(step, t0, *refs), grid=(n,),
            in_specs=[pl.BlockSpec((TM, DL), at),
                      pl.BlockSpec((C - 1, TM, DL), lambda t, t0=t0: (0, t + t0, 0)),
                      pl.BlockSpec((TM, DL), at),
                      pl.BlockSpec((MT, T, DL), lambda t, t0=t0: (t + t0, 0, 0))],
            out_specs=[],
            _explicit_indices=True,
        )(pf0, rb, xbuf.at[0], drw)
        if i == 0:
            done += [dn_forward(q) for q in rest]

    cdE = pltpu.make_async_copy(dE_v, dE_o, lsem.at[4])
    cdE.start()
    dg_cp = [start(rcopy(dg_loc, dg_all.at[r], lax.rem(r + d, G))) for d in range(1, G)]
    dg_all[r] = dg_loc[...]
    for cp in dg_cp:
        cp.wait_recv()
    cg = pltpu.make_async_copy(dg_all, dg_o, lsem.at[5])
    cg.start()
    cg.wait()
    cdE.wait()
    cdW.wait()
    for cp in sent:
        cp.wait_send()


def solution(mesh):
    G = mesh.shape['tp']

    def body(ids, E, g, W, du, dres):
        K, T = ids.shape
        D = g.shape[0]
        V, DL = E.shape
        FL = W.shape[1]
        TL = T // G
        N = K * T
        C = G // 2
        nt = N // TM
        DN = ((0, nt // 2), (nt // 2, nt // 4), (nt - nt // 4, nt // 8), (nt - nt // 8, nt // 8))
        ncp = 64 + 6 * len(DN)
        S = jax.ShapeDtypeStruct
        anyspec = pl.BlockSpec(memory_space=pl.ANY)
        vspec = pl.BlockSpec(memory_space=pltpu.VMEM)
        outs = pl.pallas_call(
            functools.partial(kernel, G, DN),
            out_shape=[S((N, FL), bf16), S((K, TL, D), bf16), S((V, DL), f32), S((D, FL), f32), S((G, 8, DL), f32),
                       S((G, N, DL), bf16), S((N, FL), bf16), S((K, T, DL), bf16), S((2, K // 2, TL, 2 * DL), bf16),
                       S((N, DL), f32), S((C - 1, N, DL), bf16), S((C - 1, N, DL), bf16), S((N, DL), bf16)],
            in_specs=[anyspec, vspec, vspec, anyspec, anyspec, anyspec, anyspec],
            out_specs=[anyspec] * 13,
            scratch_shapes=[
                pltpu.VMEM((V, DL), bf16),
                pltpu.VMEM((D, FL), bf16),
                pltpu.VMEM((C, DL, FL), bf16),
                pltpu.VMEM((D, FL), f32),
                pltpu.VMEM((V, DL), f32),
                pltpu.VMEM((N, 1), f32),
                pltpu.VMEM((TM, TM), f32),
                pltpu.VMEM((TM, FL), f32),
                pltpu.VMEM((3, TM, DL), bf16),
                pltpu.VMEM((K, TL, DL), bf16),
                pltpu.VMEM((nt, TM), f32),
                pltpu.VMEM((G - 1, nt, TM), f32),
                pltpu.VMEM((nt, TM), f32),
                pltpu.VMEM((8, DL), f32),
                pltpu.VMEM((G, 8, DL), f32),
                pltpu.SemaphoreType.DMA((6,)),
                pltpu.SemaphoreType.DMA((ncp,)),
                pltpu.SemaphoreType.DMA((ncp,)),
            ],
            compiler_params=pltpu.CompilerParams(collective_id=0, has_side_effects=True, vmem_limit_bytes=66000000),
        )(ids.reshape(N, 1), ids.reshape(nt, TM), g.astype(f32).reshape(G, DL), E, W, du.reshape(N, FL), dres)
        u, x, dE, dW, dg = outs[:5]
        return u.reshape(K, T, FL), x, dE, dW, dg[:, 0, :].reshape(D)

    return jax.shard_map(
        body,
        mesh=mesh,
        in_specs=(P('dp', None), P(None, 'tp'), P(), P(None, 'tp'), P('dp', None, 'tp'), P('dp', 'tp', None)),
        out_specs=(P('dp', None, 'tp'), P('dp', 'tp', None), P('dp', 'tp'), P('dp', 'tp'), P('dp')),
        check_vma=False,
    )
```

```python
import functools

import jax
import jax.numpy as jnp
from jax import lax
from jax.experimental import pallas as pl
from jax.experimental.pallas import tpu as pltpu
from jax.sharding import PartitionSpec as P

EPS = 1e-6
TM = 512
AHEAD = 3
LATE = 1
f32, bf16 = jnp.float32, jnp.bfloat16
MESH = pl.DeviceIdType.MESH


def id_row(ids, t, n):
    return jnp.concatenate([ids[pl.ds(t + m, 1), :] for m in range(n)], axis=1)


def tail(MT, t0, ids, d3, dg, u, x, dE, dW, u_o, x_o, dE_o, dW_o, dg_o):
    u_o[...] = u[...]
    x_o[...] = x[...]
    dW_o[...] = dW[...]
    VB = dE.shape[0]
    NL = d3.shape[1]
    it = lax.broadcasted_iota(jnp.int32, (VB, NL), 0) + pl.program_id(0) * VB
    oh = jnp.where(id_row(ids, t0, MT * NL // TM) == it, 1.0, 0.0).astype(bf16)
    a = jnp.dot(oh, d3[0], preferred_element_type=f32)
    a = a + jnp.dot(oh, d3[1], preferred_element_type=f32)
    a = a + jnp.dot(oh, d3[2], preferred_element_type=f32)
    dE_o[...] = dE[...] + a

    @pl.when(pl.program_id(0) == 0)
    def _():
        for b in range(dg.shape[0]):
            dg_o[0:1, b * dg.shape[2]:(b + 1) * dg.shape[2]] = dg[b, 0:1, :]


def kernel(G, AHEAD, LATE, ids, g8, E, W, du, dr,
           u_o, x_o, dE_o, dW_o, dg_o, d3_o,
           xbuf, dup, drw, dst, pf0, pb, rb, st,
           E_v, W_v, wp_v, dW_v, dE_v, rs_v, acc_v, accu_v, d3_v, drl_v,
           s_loc, s_rcv, sm_v, dg_loc, dg_all, lsem, ssem, rsem):
    C = G // 2
    K, TL, D = dr.shape
    N, FL = du.shape
    V, DL = E.shape
    T = TL * G
    NTILE = N // TM
    MT = TM // T
    r = lax.axis_index('tp')
    k, c = lax.div(r, 2), lax.rem(r, 2)
    mate = r + 1 - 2 * c
    right = lax.rem(r + 2, G)
    left = lax.rem(r + G - 2, G)

    def blk(o, p):
        return lax.rem(k + o, C) * 2 + (c if p == 0 else 1 - c)

    def cols(b, n=DL):
        return pl.ds(pl.multiple_of(b * DL, DL), n)

    used = [0]

    def rcopy(src, dstr, dev):
        i = used[0]
        used[0] += 1
        return pltpu.make_async_remote_copy(
            src_ref=src, dst_ref=dstr, send_sem=ssem.at[i], recv_sem=rsem.at[i],
            device_id={'tp': dev}, device_id_type=MESH)

    sent = []

    def start(cp):
        cp.start()
        sent.append(cp)
        return cp

    barrier = pltpu.get_barrier_semaphore()
    for d in range(1, G):
        pl.semaphore_signal(barrier, inc=1, device_id={'tp': lax.rem(r + d, G)}, device_id_type=MESH)
    pl.semaphore_wait(barrier, G - 1)

    rows = pl.ds(pl.multiple_of(r * TL, TL), TL)
    Kh = K // 2
    dres_in = []
    to_r = start(rcopy(dr.at[pl.ds(0, Kh), :, cols(lax.rem(k + 2, C) * 2, 2 * DL)], dst.at[0], right))
    to_l = start(rcopy(dr.at[pl.ds(Kh, Kh), :, cols(lax.rem(k + 2, C) * 2, 2 * DL)], dst.at[1], left))
    for o in (1, C - 1):
        for p in range(2):
            b = blk(o, p)
            dres_in.append(start(rcopy(dr.at[:, :, cols(b)], drw.at[:, rows, :], b)))
    dup_cp = start(rcopy(du, dup, mate))
    wp_cp = [start(rcopy(W.at[cols(blk(o, 1)), :], wp_v.at[o], mate)) for o in range(C)]
    dres_in.append(start(rcopy(dr.at[:, :, cols(mate)], drw.at[:, rows, :], mate)))

    cE = pltpu.make_async_copy(E, E_v, lsem.at[0])
    cW = pltpu.make_async_copy(W, W_v, lsem.at[1])
    cD = pltpu.make_async_copy(dr.at[:, :, cols(r)], drl_v, lsem.at[2])
    cE.start()
    cW.start()
    cD.start()
    cE.wait()

    NA = 2
    NT = N // NA
    h = NT // 2
    TA = NT // TM

    def gather(step, i, xl_b):
        acc_v[...] = jnp.zeros_like(acc_v)
        row = id_row(ids, (step.index[0] + i * TA) * MT, MT).astype(f32)
        id_b = jnp.broadcast_to(row, (128, TM)).T[:, 0:1].astype(jnp.int32)

        @pl.loop(0, V // TM)
        def _(v):
            it = lax.broadcasted_iota(jnp.int32, (TM, TM), 1) + v * TM
            oh = jnp.where(id_b == it, 1.0, 0.0).astype(bf16)
            acc_v[...] += jnp.dot(oh, E_v[pl.ds(pl.multiple_of(v * TM, TM), TM), :], preferred_element_type=f32)

        xl_b[...] = acc_v[...].astype(bf16)

    x_first = []
    for i in range(NA):
        pltpu.emit_pipeline(
            lambda step, xl_b, i=i: gather(step, i, xl_b), grid=(TA,),
            out_specs=[pl.BlockSpec((TM, DL), lambda t, i=i: (t + i * TA, 0))],
            _explicit_indices=True,
        )(xbuf.at[0])
        cs = pl.ds(i * NT, NT)
        x_first.append((
            start(rcopy(xbuf.at[0, cs], xbuf.at[6, cs], right)),
            start(rcopy(xbuf.at[0, cs], xbuf.at[2, cs], left)),
            start(rcopy(xbuf.at[0, cs], xbuf.at[1, cs], mate))))

    cD.wait()
    cD2 = pltpu.make_async_copy(drl_v, drw.at[:, rows, :], lsem.at[2])
    cD2.start()
    dW_v[...] = jnp.zeros_like(dW_v)
    dE_v[...] = jnp.zeros_like(dE_v)
    dg_loc[...] = jnp.zeros_like(dg_loc)

    to_r.wait_recv()
    rl = pl.ds(pl.multiple_of(left * TL, TL), TL)
    rr = pl.ds(pl.multiple_of(right * TL, TL), TL)
    for p in range(2):
        q = c if p == 0 else 1 - c
        dres_in.append(start(rcopy(dst.at[0, :, :, pl.ds(pl.multiple_of(q * DL, DL), DL)],
                                   drw.at[pl.ds(0, Kh), rl, :], lax.rem(k + 1, C) * 2 + q)))
    to_l.wait_recv()
    for p in range(2):
        q = c if p == 0 else 1 - c
        dres_in.append(start(rcopy(dst.at[1, :, :, pl.ds(pl.multiple_of(q * DL, DL), DL)],
                                   drw.at[pl.ds(Kh, Kh), rr, :], lax.rem(k + C - 1, C) * 2 + q)))

    cW.wait()
    dup_cp.wait_recv()
    for cp in wp_cp:
        cp.wait_recv()
    nt_dims = (((1,), (1,)), ((), ()))

    def partial(step, du_b, dp_b, p0_b, p_b):
        for o in range(C):
            w = W_v[cols(blk(o, 0)), :]
            a = lax.dot_general(du_b[...], w, nt_dims, preferred_element_type=f32)
            a = a + lax.dot_general(dp_b[...], wp_v[o], nt_dims, preferred_element_type=f32)
            if o == 0:
                p0_b[...] = a
            else:
                p_b[o - 1, 0] = a.astype(bf16)

    tile = lambda t: (t, 0)
    pltpu.emit_pipeline(
        partial, grid=(NTILE,),
        in_specs=[pl.BlockSpec((TM, FL), tile), pl.BlockSpec((TM, FL), tile)],
        out_specs=[pl.BlockSpec((TM, DL), tile), pl.BlockSpec((C - 1, 1, TM, DL), lambda t: (0, t, 0, 0))],
        _explicit_indices=True,
    )(du, dup, pf0, pb)

    x_second, x_mate = [], []
    for i in range(NA):
        fr, fl, _ = x_first[i]
        lo, hi = pl.ds(i * NT, h), pl.ds(i * NT + h, h)
        cs = pl.ds(i * NT, NT)
        fr.wait_recv()
        a = start(rcopy(xbuf.at[6, lo], xbuf.at[4, lo], right))
        m6 = start(rcopy(xbuf.at[6, cs], xbuf.at[7, cs], mate))
        fl.wait_recv()
        b = start(rcopy(xbuf.at[2, hi], xbuf.at[4, hi], left))
        m2 = start(rcopy(xbuf.at[2, cs], xbuf.at[3, cs], mate))
        x_second.append((a, b))
        x_mate.append([m6, m2])

    TH = TM // 2
    tlo, thi = pl.ds(0, TH), pl.ds(TH, TH)
    across = []
    NG = NTILE // 2
    for q in range(2):
        gs = pl.ds(q * NG, NG)
        across.append((start(rcopy(pb.at[1, gs, tlo], st.at[gs, tlo], right)),
                       start(rcopy(pb.at[1, gs, thi], st.at[gs, thi], left))))

    def dn_send(t):
        return (start(rcopy(pb.at[0, t], rb.at[2, t], right)),
                start(rcopy(pb.at[2, t], rb.at[0, t], left)))

    def dn_forward(t):
        return (start(rcopy(st.at[t, tlo], rb.at[1, t, tlo], right)),
                start(rcopy(st.at[t, thi], rb.at[1, t, thi], left)))

    near = [dn_send(t) for t in range(AHEAD)]

    t_dims = (((0,), (0,)), ((), ()))

    def forward(step, i, x_b, du_b, u_b, xo_b):
        t = step.index[0] + i * TA
        rs_v[pl.ds(pl.multiple_of(t * TM, TM), TM), :] = jnp.zeros((TM, 1), f32)
        here = pl.ds(pl.multiple_of(t * TM, TM), TM)

        @pl.loop(0, G)
        def _(j):
            x = x_b[j].astype(f32)
            rs_v[here, :] += jnp.sum(x * x, axis=-1, keepdims=True)

        rs_v[here, :] = lax.rsqrt(rs_v[here, :] / D + EPS)
        accu_v[...] = jnp.zeros_like(accu_v)

        @pl.loop(0, G)
        def _(j):
            p = lax.rem(j, 2)
            b = lax.rem(k + lax.div(j, 2), C) * 2 + c + p - 2 * c * p
            n = ((x_b[j].astype(f32) * rs_v[here, :]) * g8[pl.ds(b, 1), :]).astype(bf16)
            accu_v[...] += jnp.dot(n, W_v[cols(b), :], preferred_element_type=f32)
            dW_v[cols(b), :] += lax.dot_general(n, du_b[...], t_dims, preferred_element_type=f32)
            for m in range(MT):
                xo_b[m, :, cols(b)] = x_b[j, pl.ds(pl.multiple_of(m * T + r * TL, TL), TL), :]

        uf = accu_v[...]
        u_b[...] = uf.astype(bf16)
        s = jnp.sum(uf * du_b[...].astype(f32), axis=-1, keepdims=True)
        s_loc[pl.ds(t, 1), :] = jnp.broadcast_to(s, (TM, 128)).T[0:1, :]

    for i in range(NA):
        a, b = x_second[i]
        lo, hi = pl.ds(i * NT, h), pl.ds(i * NT + h, h)
        a.wait_recv()
        m4a = start(rcopy(xbuf.at[4, lo], xbuf.at[5, lo], mate))
        b.wait_recv()
        m4b = start(rcopy(xbuf.at[4, hi], xbuf.at[5, hi], mate))
        x_first[i][2].wait_recv()
        for cp in x_mate[i]:
            cp.wait_recv()
        m4a.wait_recv()
        m4b.wait_recv()
        at = lambda t, i=i: (t + i * TA, 0)
        pltpu.emit_pipeline(
            lambda step, *refs, i=i: forward(step, i, *refs), grid=(TA,),
            in_specs=[pl.BlockSpec((G, TM, DL), lambda t, i=i: (0, t + i * TA, 0)), pl.BlockSpec((TM, FL), at)],
            out_specs=[pl.BlockSpec((TM, FL), at), pl.BlockSpec((MT, TL, D), lambda t, i=i: (t + i * TA, 0, 0))],
            _explicit_indices=True,
        )(xbuf, du, u_o, x_o)

    cdW = pltpu.make_async_copy(dW_v, dW_o, lsem.at[3])
    cdW.start()
    s_cp = [start(rcopy(s_loc, s_rcv.at[G - d - 1], lax.rem(r + d, G))) for d in range(1, G)]
    for cp in across[0]:
        cp.wait_recv()
    far = [dn_forward(t) for t in range(AHEAD)]
    for cp in s_cp:
        cp.wait_recv()
    tot = jnp.zeros_like(s_loc)
    for dev in range(G):
        d = lax.rem(dev - r + G, G)
        other = s_rcv[lax.max(d - 1, 0)]
        tot = tot + jnp.where(d == 0, s_loc[...], other)
    sm_v[...] = tot / D
    for cp in across[1]:
        cp.wait_recv()
    cD2.wait()
    for cp in dres_in:
        cp.wait_recv()

    def backward(step, t0, p0_b, rb_b, xl_b, dr_b, *late):
        t = step.index[0] + t0
        here = pl.ds(pl.multiple_of(t * TM, TM), TM)
        dn = (p0_b[...] + rb_b[0, 0].astype(f32)) + (rb_b[1, 0].astype(f32) + rb_b[2, 0].astype(f32))
        rs = rs_v[here, :]
        s = jnp.broadcast_to(sm_v[pl.ds(t, 1), :], (128, TM)).T[:, 0:1]
        nh = xl_b[...].astype(f32) * rs
        dx = dr_b[...].reshape(TM, DL).astype(f32) + rs * (g8[pl.ds(r, 1), :] * dn - nh * s)
        dg_loc[0:1, :] += jnp.sum(dn * nh, axis=0, keepdims=True)
        hi = dx.astype(bf16)
        e1 = dx - hi.astype(f32)
        md = e1.astype(bf16)
        to = late[0] if late else d3_v
        to[0] = hi
        to[1] = md
        to[2] = (e1 - md.astype(f32)).astype(bf16)
        if late:
            return

        row = id_row(ids, t * MT, MT)

        @pl.loop(0, V // TM)
        def _(v):
            it = lax.broadcasted_iota(jnp.int32, (TM, TM), 0) + v * TM
            oh = jnp.where(row == it, 1.0, 0.0).astype(bf16)
            a = jnp.dot(oh, d3_v[0], preferred_element_type=f32)
            a = a + jnp.dot(oh, d3_v[1], preferred_element_type=f32)
            a = a + jnp.dot(oh, d3_v[2], preferred_element_type=f32)
            dE_v[pl.ds(pl.multiple_of(v * TM, TM), TM), :] += a

    for i in range(NTILE):
        for cp in near[i] + far[i]:
            cp.wait_recv()
        if i + AHEAD < NTILE:
            near.append(dn_send(i + AHEAD))
            far.append(dn_forward(i + AHEAD))
        late = i >= NTILE - LATE
        at = lambda t, i=i: (t + i, 0)
        pltpu.emit_pipeline(
            lambda step, *refs, i=i: backward(step, i, *refs), grid=(1,),
            in_specs=[pl.BlockSpec((TM, DL), at),
                      pl.BlockSpec((C - 1, 1, TM, DL), lambda t, i=i: (0, t + i, 0, 0)),
                      pl.BlockSpec((TM, DL), at),
                      pl.BlockSpec((MT, T, DL), lambda t, i=i: (t + i, 0, 0))],
            out_specs=[pl.BlockSpec((3, TM, DL), lambda t, i=i: (0, t + i - (NTILE - LATE), 0))] if late else [],
            _explicit_indices=True,
        )(*([pf0, rb, xbuf.at[0], drw] + ([d3_o] if late else [])))
        if i == NTILE - LATE - 1:
            cdE = pltpu.make_async_copy(dE_v, dE_o, lsem.at[4])
            cdE.start()

    dg_cp = [start(rcopy(dg_loc, dg_all.at[r], lax.rem(r + d, G))) for d in range(1, G)]
    dg_all[r] = dg_loc[...]
    for cp in dg_cp:
        cp.wait_recv()
    cg = pltpu.make_async_copy(dg_all, dg_o, lsem.at[5])
    cg.start()
    cg.wait()
    cdE.wait()
    cdW.wait()
    for cp in sent:
        cp.wait_send()


def solution(mesh):
    G = mesh.shape['tp']

    def body(ids, E, g, W, du, dres):
        K, T = ids.shape
        D = g.shape[0]
        V, DL = E.shape
        FL = W.shape[1]
        TL = T // G
        N = K * T
        C = G // 2
        nt = N // TM
        NL = LATE * TM
        ncp = 64 + 4 * nt
        S = jax.ShapeDtypeStruct
        anyspec = pl.BlockSpec(memory_space=pl.ANY)
        vspec = pl.BlockSpec(memory_space=pltpu.VMEM)
        outs = pl.pallas_call(
            functools.partial(kernel, G, AHEAD, LATE),
            out_shape=[S((N, FL), bf16), S((K, TL, D), bf16), S((V, DL), f32), S((D, FL), f32), S((G, 8, DL), f32),
                       S((3, NL, DL), bf16),
                       S((G, N, DL), bf16), S((N, FL), bf16), S((K, T, DL), bf16), S((2, K // 2, TL, 2 * DL), bf16),
                       S((N, DL), f32), S((C - 1, nt, TM, DL), bf16), S((C - 1, nt, TM, DL), bf16), S((nt, TM, DL), bf16)],
            in_specs=[vspec, vspec, anyspec, anyspec, anyspec, anyspec],
            out_specs=[anyspec] * 14,
            scratch_shapes=[
                pltpu.VMEM((V, DL), bf16),
                pltpu.VMEM((D, FL), bf16),
                pltpu.VMEM((C, DL, FL), bf16),
                pltpu.VMEM((D, FL), f32),
                pltpu.VMEM((V, DL), f32),
                pltpu.VMEM((N, 1), f32),
                pltpu.VMEM((TM, TM), f32),
                pltpu.VMEM((TM, FL), f32),
                pltpu.VMEM((3, TM, DL), bf16),
                pltpu.VMEM((K, TL, DL), bf16),
                pltpu.VMEM((nt, TM), f32),
                pltpu.VMEM((G - 1, nt, TM), f32),
                pltpu.VMEM((nt, TM), f32),
                pltpu.VMEM((8, DL), f32),
                pltpu.VMEM((G, 8, DL), f32),
                pltpu.SemaphoreType.DMA((6,)),
                pltpu.SemaphoreType.DMA((ncp,)),
                pltpu.SemaphoreType.DMA((ncp,)),
            ],
            compiler_params=pltpu.CompilerParams(collective_id=0, has_side_effects=True, vmem_limit_bytes=66000000),
        )(ids, g.astype(f32).reshape(G, DL), E, W, du.reshape(N, FL), dres)
        u, x, dE, dW, dg, d3 = outs[:6]
        rowblk = lambda n, m: pl.BlockSpec((2 * n // K, m), lambda i: (i, 0))
        blocks = [rowblk(N, FL), pl.BlockSpec((2, TL, D), lambda i: (i, 0, 0)), rowblk(V, DL), rowblk(D, FL)]
        u, x, dE, dW, dg = pl.pallas_call(
            functools.partial(tail, TM // T, (nt - LATE) * TM // T),
            grid=(K // 2,),
            out_shape=[S((N, FL), bf16), S((K, TL, D), bf16), S((V, DL), f32), S((D, FL), f32), S((1, D), f32)],
            in_specs=[vspec, vspec, vspec] + blocks,
            out_specs=blocks + [pl.BlockSpec((1, D), lambda i: (0, 0))],
        )(ids, d3, dg, u, x, dE, dW)
        return u.reshape(K, T, FL), x, dE, dW, dg.reshape(D)

    return jax.shard_map(
        body,
        mesh=mesh,
        in_specs=(P('dp', None), P(None, 'tp'), P(), P(None, 'tp'), P('dp', None, 'tp'), P('dp', 'tp', None)),
        out_specs=(P('dp', None, 'tp'), P('dp', 'tp', None), P('dp', 'tp'), P('dp', 'tp'), P('dp')),
        check_vma=False,
    )
```

```python
import functools

import jax
import jax.numpy as jnp
from jax import lax
from jax.experimental import pallas as pl
from jax.experimental.pallas import tpu as pltpu
from jax.sharding import PartitionSpec as P

EPS = 1e-6
TM = 512
AHEAD = 3
VLIM = 41 << 20
VTAIL = 18 << 20
f32, bf16 = jnp.float32, jnp.bfloat16
MESH = pl.DeviceIdType.MESH


def id_row(ids, t, n):
    return jnp.concatenate([ids[pl.ds(t + m, 1), :] for m in range(n)], axis=1)


def tail(MT, t0, ids, d3, dg, u, x, dE, dW, u_o, x_o, dE_o, dg_o, dW_o, sem):
    out = pltpu.make_async_copy(dW, dW_o, sem)

    @pl.when(pl.program_id(0) == 0)
    def _():
        out.start()

    u_o[...] = u[...]
    x_o[...] = x[...]
    i = pl.program_id(0)
    VB = dE_o.shape[0]
    NL = d3.shape[1]
    it = lax.broadcasted_iota(jnp.int32, (VB, NL), 0) + i * VB
    oh = jnp.where(id_row(ids, t0, MT * NL // TM) == it, 1.0, 0.0).astype(bf16)
    a = jnp.dot(oh, d3[0], preferred_element_type=f32)
    a = a + jnp.dot(oh, d3[1], preferred_element_type=f32)
    a = a + jnp.dot(oh, d3[2], preferred_element_type=f32)
    dE_o[...] = dE[pl.ds(pl.multiple_of(i * VB, VB), VB), :] + a

    @pl.when(pl.program_id(0) == 0)
    def _():
        for b in range(dg.shape[0]):
            dg_o[0:1, b * dg.shape[2]:(b + 1) * dg.shape[2]] = dg[b, 0:1, :]

    @pl.when(pl.program_id(0) == pl.num_programs(0) - 1)
    def _():
        out.wait()


def kernel(G, AHEAD, ids, g8, E, W, du, dr,
           u_o, x_o, dE_v, dW_v, dg_o, d3_v,
           xbuf, dup, drw, dst, pf0, pb, rb, st,
           E_v, W_v, wp_v, rs_v, acc_v, accu_v, drl_v,
           s_loc, s_rcv, sm_v, dg_loc, dg_all, lsem, ssem, rsem):
    C = G // 2
    K, TL, D = dr.shape
    N, FL = du.shape
    V, DL = E.shape
    T = TL * G
    NTILE = N // TM
    MT = TM // T
    r = lax.axis_index('tp')
    k, c = lax.div(r, 2), lax.rem(r, 2)
    mate = r + 1 - 2 * c
    right = lax.rem(r + 2, G)
    left = lax.rem(r + G - 2, G)

    def blk(o, p):
        return lax.rem(k + o, C) * 2 + (c if p == 0 else 1 - c)

    def cols(b, n=DL):
        return pl.ds(pl.multiple_of(b * DL, DL), n)

    used = [0]

    def rcopy(src, dstr, dev):
        i = used[0]
        used[0] += 1
        return pltpu.make_async_remote_copy(
            src_ref=src, dst_ref=dstr, send_sem=ssem.at[i], recv_sem=rsem.at[i],
            device_id={'tp': dev}, device_id_type=MESH)

    sent = []

    def start(cp):
        cp.start()
        sent.append(cp)
        return cp

    barrier = pltpu.get_barrier_semaphore()
    for d in range(1, G):
        pl.semaphore_signal(barrier, inc=1, device_id={'tp': lax.rem(r + d, G)}, device_id_type=MESH)
    pl.semaphore_wait(barrier, G - 1)

    rows = pl.ds(pl.multiple_of(r * TL, TL), TL)
    Kh = K // 2
    dres_in = []
    to_r = start(rcopy(dr.at[pl.ds(0, Kh), :, cols(lax.rem(k + 2, C) * 2, 2 * DL)], dst.at[0], right))
    to_l = start(rcopy(dr.at[pl.ds(Kh, Kh), :, cols(lax.rem(k + 2, C) * 2, 2 * DL)], dst.at[1], left))
    for o in (1, C - 1):
        for p in range(2):
            b = blk(o, p)
            dres_in.append(start(rcopy(dr.at[:, :, cols(b)], drw.at[:, rows, :], b)))
    dup_cp = start(rcopy(du, dup, mate))
    wp_cp = [start(rcopy(W.at[cols(blk(o, 1)), :], wp_v.at[o], mate)) for o in range(C)]
    dres_in.append(start(rcopy(dr.at[:, :, cols(mate)], drw.at[:, rows, :], mate)))

    cE = pltpu.make_async_copy(E, E_v, lsem.at[0])
    cW = pltpu.make_async_copy(W, W_v, lsem.at[1])
    cD = pltpu.make_async_copy(dr.at[:, :, cols(r)], drl_v, lsem.at[2])
    cE.start()
    cW.start()
    cD.start()
    cE.wait()

    NA = 2
    NT = N // NA
    h = NT // 2
    TA = NT // TM

    def gather(step, i, xl_b):
        acc_v[...] = jnp.zeros_like(acc_v)
        row = id_row(ids, (step.index[0] + i * TA) * MT, MT).astype(f32)
        id_b = jnp.broadcast_to(row, (128, TM)).T[:, 0:1].astype(jnp.int32)

        @pl.loop(0, V // TM)
        def _(v):
            it = lax.broadcasted_iota(jnp.int32, (TM, TM), 1) + v * TM
            oh = jnp.where(id_b == it, 1.0, 0.0).astype(bf16)
            acc_v[...] += jnp.dot(oh, E_v[pl.ds(pl.multiple_of(v * TM, TM), TM), :], preferred_element_type=f32)

        xl_b[...] = acc_v[...].astype(bf16)

    x_first = []
    for i in range(NA):
        pltpu.emit_pipeline(
            lambda step, xl_b, i=i: gather(step, i, xl_b), grid=(TA,),
            out_specs=[pl.BlockSpec((TM, DL), lambda t, i=i: (t + i * TA, 0))],
            _explicit_indices=True,
        )(xbuf.at[0])
        cs = pl.ds(i * NT, NT)
        x_first.append((
            start(rcopy(xbuf.at[0, cs], xbuf.at[6, cs], right)),
            start(rcopy(xbuf.at[0, cs], xbuf.at[2, cs], left)),
            start(rcopy(xbuf.at[0, cs], xbuf.at[1, cs], mate))))

    cD.wait()
    cD2 = pltpu.make_async_copy(drl_v, drw.at[:, rows, :], lsem.at[2])
    cD2.start()
    dW_v[...] = jnp.zeros_like(dW_v)
    dE_v[...] = jnp.zeros_like(dE_v)
    dg_loc[...] = jnp.zeros_like(dg_loc)

    to_r.wait_recv()
    rl = pl.ds(pl.multiple_of(left * TL, TL), TL)
    rr = pl.ds(pl.multiple_of(right * TL, TL), TL)
    for p in range(2):
        q = c if p == 0 else 1 - c
        dres_in.append(start(rcopy(dst.at[0, :, :, pl.ds(pl.multiple_of(q * DL, DL), DL)],
                                   drw.at[pl.ds(0, Kh), rl, :], lax.rem(k + 1, C) * 2 + q)))
    to_l.wait_recv()
    for p in range(2):
        q = c if p == 0 else 1 - c
        dres_in.append(start(rcopy(dst.at[1, :, :, pl.ds(pl.multiple_of(q * DL, DL), DL)],
                                   drw.at[pl.ds(Kh, Kh), rr, :], lax.rem(k + C - 1, C) * 2 + q)))

    cW.wait()
    dup_cp.wait_recv()
    for cp in wp_cp:
        cp.wait_recv()
    nt_dims = (((1,), (1,)), ((), ()))

    def partial(step, du_b, dp_b, p0_b, p_b):
        for o in range(C):
            w = W_v[cols(blk(o, 0)), :]
            a = lax.dot_general(du_b[...], w, nt_dims, preferred_element_type=f32)
            a = a + lax.dot_general(dp_b[...], wp_v[o], nt_dims, preferred_element_type=f32)
            if o == 0:
                p0_b[...] = a
            else:
                p_b[o - 1, 0] = a.astype(bf16)

    tile = lambda t: (t, 0)
    pltpu.emit_pipeline(
        partial, grid=(NTILE,),
        in_specs=[pl.BlockSpec((TM, FL), tile), pl.BlockSpec((TM, FL), tile)],
        out_specs=[pl.BlockSpec((TM, DL), tile), pl.BlockSpec((C - 1, 1, TM, DL), lambda t: (0, t, 0, 0))],
        _explicit_indices=True,
    )(du, dup, pf0, pb)

    x_second, x_mate = [], []
    for i in range(NA):
        fr, fl, _ = x_first[i]
        lo, hi = pl.ds(i * NT, h), pl.ds(i * NT + h, h)
        cs = pl.ds(i * NT, NT)
        fr.wait_recv()
        a = start(rcopy(xbuf.at[6, lo], xbuf.at[4, lo], right))
        m6 = start(rcopy(xbuf.at[6, cs], xbuf.at[7, cs], mate))
        fl.wait_recv()
        b = start(rcopy(xbuf.at[2, hi], xbuf.at[4, hi], left))
        m2 = start(rcopy(xbuf.at[2, cs], xbuf.at[3, cs], mate))
        x_second.append((a, b))
        x_mate.append([m6, m2])

    TH = TM // 2
    tlo, thi = pl.ds(0, TH), pl.ds(TH, TH)
    across = []
    NG = NTILE // 2
    for q in range(2):
        gs = pl.ds(q * NG, NG)
        across.append((start(rcopy(pb.at[1, gs, tlo], st.at[gs, tlo], right)),
                       start(rcopy(pb.at[1, gs, thi], st.at[gs, thi], left))))

    def dn_send(t):
        return (start(rcopy(pb.at[0, t], rb.at[2, t], right)),
                start(rcopy(pb.at[2, t], rb.at[0, t], left)))

    def dn_forward(t):
        return (start(rcopy(st.at[t, tlo], rb.at[1, t, tlo], right)),
                start(rcopy(st.at[t, thi], rb.at[1, t, thi], left)))

    near = [dn_send(t) for t in range(AHEAD)]

    t_dims = (((0,), (0,)), ((), ()))

    def forward(step, i, x_b, du_b, u_b, xo_b):
        t = step.index[0] + i * TA
        rs_v[pl.ds(pl.multiple_of(t * TM, TM), TM), :] = jnp.zeros((TM, 1), f32)
        here = pl.ds(pl.multiple_of(t * TM, TM), TM)

        @pl.loop(0, G)
        def _(j):
            x = x_b[j].astype(f32)
            rs_v[here, :] += jnp.sum(x * x, axis=-1, keepdims=True)

        rs_v[here, :] = lax.rsqrt(rs_v[here, :] / D + EPS)
        accu_v[...] = jnp.zeros_like(accu_v)

        @pl.loop(0, G)
        def _(j):
            p = lax.rem(j, 2)
            b = lax.rem(k + lax.div(j, 2), C) * 2 + c + p - 2 * c * p
            n = ((x_b[j].astype(f32) * rs_v[here, :]) * g8[pl.ds(b, 1), :]).astype(bf16)
            accu_v[...] += jnp.dot(n, W_v[cols(b), :], preferred_element_type=f32)
            dW_v[cols(b), :] += lax.dot_general(n, du_b[...], t_dims, preferred_element_type=f32)
            for m in range(MT):
                xo_b[m, :, cols(b)] = x_b[j, pl.ds(pl.multiple_of(m * T + r * TL, TL), TL), :]

        uf = accu_v[...]
        u_b[...] = uf.astype(bf16)
        s = jnp.sum(uf * du_b[...].astype(f32), axis=-1, keepdims=True)
        s_loc[pl.ds(t, 1), :] = jnp.broadcast_to(s, (TM, 128)).T[0:1, :]

    for i in range(NA):
        a, b = x_second[i]
        lo, hi = pl.ds(i * NT, h), pl.ds(i * NT + h, h)
        a.wait_recv()
        m4a = start(rcopy(xbuf.at[4, lo], xbuf.at[5, lo], mate))
        b.wait_recv()
        m4b = start(rcopy(xbuf.at[4, hi], xbuf.at[5, hi], mate))
        x_first[i][2].wait_recv()
        for cp in x_mate[i]:
            cp.wait_recv()
        m4a.wait_recv()
        m4b.wait_recv()
        at = lambda t, i=i: (t + i * TA, 0)
        pltpu.emit_pipeline(
            lambda step, *refs, i=i: forward(step, i, *refs), grid=(TA,),
            in_specs=[pl.BlockSpec((G, TM, DL), lambda t, i=i: (0, t + i * TA, 0)), pl.BlockSpec((TM, FL), at)],
            out_specs=[pl.BlockSpec((TM, FL), at), pl.BlockSpec((MT, TL, D), lambda t, i=i: (t + i * TA, 0, 0))],
            _explicit_indices=True,
        )(xbuf, du, u_o, x_o)

    s_cp = [start(rcopy(s_loc, s_rcv.at[G - d - 1], lax.rem(r + d, G))) for d in range(1, G)]
    for cp in across[0]:
        cp.wait_recv()
    far = [dn_forward(t) for t in range(AHEAD)]
    for cp in s_cp:
        cp.wait_recv()
    tot = jnp.zeros_like(s_loc)
    for dev in range(G):
        d = lax.rem(dev - r + G, G)
        other = s_rcv[lax.max(d - 1, 0)]
        tot = tot + jnp.where(d == 0, s_loc[...], other)
    sm_v[...] = tot / D
    for cp in across[1]:
        cp.wait_recv()
    cD2.wait()
    for cp in dres_in:
        cp.wait_recv()

    def backward(step, t0, late, p0_b, rb_b, xl_b, dr_b):
        t = step.index[0] + t0
        here = pl.ds(pl.multiple_of(t * TM, TM), TM)
        dn = (p0_b[...] + rb_b[0, 0].astype(f32)) + (rb_b[1, 0].astype(f32) + rb_b[2, 0].astype(f32))
        rs = rs_v[here, :]
        s = jnp.broadcast_to(sm_v[pl.ds(t, 1), :], (128, TM)).T[:, 0:1]
        nh = xl_b[...].astype(f32) * rs
        dx = dr_b[...].reshape(TM, DL).astype(f32) + rs * (g8[pl.ds(r, 1), :] * dn - nh * s)
        dg_loc[0:1, :] += jnp.sum(dn * nh, axis=0, keepdims=True)
        hi = dx.astype(bf16)
        e1 = dx - hi.astype(f32)
        md = e1.astype(bf16)
        d3_v[0] = hi
        d3_v[1] = md
        d3_v[2] = (e1 - md.astype(f32)).astype(bf16)
        if late:
            return

        row = id_row(ids, t * MT, MT)

        @pl.loop(0, V // TM)
        def _(v):
            it = lax.broadcasted_iota(jnp.int32, (TM, TM), 0) + v * TM
            oh = jnp.where(row == it, 1.0, 0.0).astype(bf16)
            a = jnp.dot(oh, d3_v[0], preferred_element_type=f32)
            a = a + jnp.dot(oh, d3_v[1], preferred_element_type=f32)
            a = a + jnp.dot(oh, d3_v[2], preferred_element_type=f32)
            dE_v[pl.ds(pl.multiple_of(v * TM, TM), TM), :] += a

    for i in range(NTILE):
        for cp in near[i] + far[i]:
            cp.wait_recv()
        if i + AHEAD < NTILE:
            near.append(dn_send(i + AHEAD))
            far.append(dn_forward(i + AHEAD))
        late = i == NTILE - 1
        at = lambda t, i=i: (t + i, 0)
        pltpu.emit_pipeline(
            lambda step, *refs, i=i, late=late: backward(step, i, late, *refs), grid=(1,),
            in_specs=[pl.BlockSpec((TM, DL), at),
                      pl.BlockSpec((C - 1, 1, TM, DL), lambda t, i=i: (0, t + i, 0, 0)),
                      pl.BlockSpec((TM, DL), at),
                      pl.BlockSpec((MT, T, DL), lambda t, i=i: (t + i, 0, 0))],
            out_specs=[],
            _explicit_indices=True,
        )(pf0, rb, xbuf.at[0], drw)

    dg_cp = [start(rcopy(dg_loc, dg_all.at[r], lax.rem(r + d, G))) for d in range(1, G)]
    dg_all[r] = dg_loc[...]
    for cp in dg_cp:
        cp.wait_recv()
    dg_o[...] = dg_all[...]
    for cp in sent:
        cp.wait_send()


def solution(mesh):
    G = mesh.shape['tp']

    def body(ids, E, g, W, du, dres):
        K, T = ids.shape
        D = g.shape[0]
        V, DL = E.shape
        FL = W.shape[1]
        TL = T // G
        N = K * T
        C = G // 2
        nt = N // TM
        ncp = 64 + 4 * nt
        S = jax.ShapeDtypeStruct
        anyspec = pl.BlockSpec(memory_space=pl.ANY)
        vspec = pl.BlockSpec(memory_space=pltpu.VMEM)
        outs = pl.pallas_call(
            functools.partial(kernel, G, AHEAD),
            out_shape=[S((N, FL), bf16), S((K, TL, D), bf16), pltpu.VMEM((V, DL), f32), pltpu.VMEM((D, FL), f32), pltpu.VMEM((G, 8, DL), f32),
                       pltpu.VMEM((3, TM, DL), bf16),
                       S((G, N, DL), bf16), S((N, FL), bf16), S((K, T, DL), bf16), S((2, K // 2, TL, 2 * DL), bf16),
                       S((N, DL), f32), S((C - 1, nt, TM, DL), bf16), S((C - 1, nt, TM, DL), bf16), S((nt, TM, DL), bf16)],
            in_specs=[vspec, vspec, anyspec, anyspec, anyspec, anyspec],
            out_specs=[anyspec] * 2 + [vspec] * 4 + [anyspec] * 8,
            scratch_shapes=[
                pltpu.VMEM((V, DL), bf16),
                pltpu.VMEM((D, FL), bf16),
                pltpu.VMEM((C, DL, FL), bf16),
                pltpu.VMEM((N, 1), f32),
                pltpu.VMEM((TM, TM), f32),
                pltpu.VMEM((TM, FL), f32),
                pltpu.VMEM((K, TL, DL), bf16),
                pltpu.VMEM((nt, TM), f32),
                pltpu.VMEM((G - 1, nt, TM), f32),
                pltpu.VMEM((nt, TM), f32),
                pltpu.VMEM((8, DL), f32),
                pltpu.VMEM((G, 8, DL), f32),
                pltpu.SemaphoreType.DMA((3,)),
                pltpu.SemaphoreType.DMA((ncp,)),
                pltpu.SemaphoreType.DMA((ncp,)),
            ],
            compiler_params=pltpu.CompilerParams(collective_id=0, has_side_effects=True, vmem_limit_bytes=VLIM),
        )(ids, g.astype(f32).reshape(G, DL), E, W, du.reshape(N, FL), dres)
        u, x, dE, dW, dg, d3 = outs[:6]
        rowblk = lambda n, m: pl.BlockSpec((2 * n // K, m), lambda i: (i, 0))
        blocks = [rowblk(N, FL), pl.BlockSpec((2, TL, D), lambda i: (i, 0, 0)), rowblk(V, DL)]
        hbm = lambda a: pltpu.with_memory_space_constraint(a, pltpu.HBM)
        vmem = lambda a: pltpu.with_memory_space_constraint(a, pltpu.VMEM)
        u, x, dE, dg, dW = pl.pallas_call(
            functools.partial(tail, TM // T, (nt - 1) * TM // T),
            grid=(K // 2,),
            out_shape=[S((N, FL), bf16), S((K, TL, D), bf16), S((V, DL), f32), S((1, D), f32), S((D, FL), f32)],
            in_specs=[vspec, vspec, vspec] + blocks[:2] + [vspec, vspec],
            scratch_shapes=[pltpu.SemaphoreType.DMA],
            compiler_params=pltpu.CompilerParams(vmem_limit_bytes=VTAIL),
            out_specs=blocks + [pl.BlockSpec((1, D), lambda i: (0, 0)), anyspec],
        )(ids, vmem(d3), vmem(dg), hbm(u), hbm(x), vmem(dE), vmem(dW))
        return u.reshape(K, T, FL), x, dE, dW, dg.reshape(D)

    return jax.shard_map(
        body,
        mesh=mesh,
        in_specs=(P('dp', None), P(None, 'tp'), P(), P(None, 'tp'), P('dp', None, 'tp'), P('dp', 'tp', None)),
        out_specs=(P('dp', None, 'tp'), P('dp', 'tp', None), P('dp', 'tp'), P('dp', 'tp'), P('dp')),
        check_vma=False,
    )
```
